16 devices in a mesh: dp: 2 (over z), vp: 8 (over y, x, core).
Axes of the slice: x: 2, y: 2, z: 2, core: 2. Of those that a mesh axis runs over, the one named last changes fastest.
Arguments:
- hidden: bfloat16 [2, 4096, 2560], P('dp', 'vp')
- targets: int32 [2, 4096], P('dp', 'vp')
- loss_mask: int32 [2, 4096], P('dp', 'vp')
- norm_scale: float32 [2560], replicated
- w_head: bfloat16 [2560, 65536], P(None, 'vp')
Outputs:
- output 1: float32 [], replicated
- output 2: bfloat16 [2, 4096, 2560], P('dp', 'vp')
- output 3: float32 [2560, 65536], P(None, 'vp')
- output 4: float32 [2560], replicated
All inputs are finite; a program needn't handle non-finite values.
Results may differ from the reference program's by a relative error of at most 0.001.
Values sent between devices are 32-bit elements.
A program may use at most 1 GiB of HBM per device.

```python
import jax
import jax.numpy as jnp
import math
from jax import lax

MODEL_DIM = 2560
VOCAB_SIZE = 65536
DP_SIZE = 2
VP_SIZE = 8
BATCH_DEV = 1
TOK_DEV = 512

EPS = 1e-5
VOCAB_PAD = ((VOCAB_SIZE + 128 * VP_SIZE - 1) // (128 * VP_SIZE)) * 128 * VP_SIZE
BATCH = DP_SIZE * BATCH_DEV
SEQ_LEN = VP_SIZE * TOK_DEV


def setup_inputs(seed: int = 0) -> dict:
    key = jax.random.key(seed)
    k_hid, k_tgt, k_pct, k_msk, k_scale, k_w, k_col, k_blk = jax.random.split(key, 8)
    hidden = jax.random.normal(k_hid, (BATCH, SEQ_LEN, MODEL_DIM), jnp.float32).astype(jnp.bfloat16)
    targets = jax.random.randint(k_tgt, (BATCH, SEQ_LEN), 0, VOCAB_SIZE, jnp.int32)
    targets = targets.at[0, 0].set(0).at[BATCH - 1, SEQ_LEN - 1].set(VOCAB_SIZE - 1)
    keep_pct = jnp.repeat(jax.random.randint(k_pct, (DP_SIZE,), 10, 96, jnp.int32), BATCH_DEV)
    draws = jax.random.randint(k_msk, (BATCH, SEQ_LEN), 0, 100, jnp.int32)
    loss_mask = (draws < keep_pct[:, None]).astype(jnp.int32)
    loss_mask = loss_mask.at[0, 0].set(1).at[0, 1].set(0)
    norm_scale = jax.random.uniform(k_scale, (MODEL_DIM,), jnp.float32, 0.5, 1.5)
    col_scale = jnp.exp(0.35 * jax.random.normal(k_col, (VOCAB_PAD,), jnp.float32))
    blk_scale = jnp.repeat(jnp.exp(0.3 * jax.random.normal(k_blk, (VOCAB_PAD // 128,), jnp.float32)), 128)
    fan_scale = 1.0 / math.sqrt(MODEL_DIM)
    w_f32 = jax.random.normal(k_w, (MODEL_DIM, VOCAB_PAD), jnp.float32) * fan_scale
    w_head = (w_f32 * (col_scale * blk_scale)).astype(jnp.bfloat16)
    return {'hidden': hidden, 'targets': targets, 'loss_mask': loss_mask, 'norm_scale': norm_scale, 'w_head': w_head}


def rms_norm(x_rows, norm_scale):
    inv_rms = lax.rsqrt(jnp.mean(x_rows * x_rows, axis=-1, keepdims=True) + EPS)
    return x_rows * inv_rms * norm_scale


def reference(hidden, targets, loss_mask, norm_scale, w_head):
    num_blocks = BATCH * SEQ_LEN // TOK_DEV
    mask_f = loss_mask.astype(jnp.float32)
    tok_weight = (mask_f / jnp.sum(mask_f)).reshape(num_blocks, TOK_DEV)
    x_blocks = hidden.reshape(num_blocks, TOK_DEV, MODEL_DIM)
    tgt_blocks = targets.reshape(num_blocks, TOK_DEV)
    col_ids = lax.broadcasted_iota(jnp.int32, (1, VOCAB_PAD), 1)

    def block_step(carried, block_in):
        loss_acc, dscale_acc, dw_acc = carried
        x_blk, tgt_blk, wt_blk = block_in
        normed_f, norm_vjp = jax.vjp(rms_norm, x_blk.astype(jnp.float32), norm_scale)
        normed = normed_f.astype(jnp.bfloat16)
        logits = jnp.dot(normed, w_head, preferred_element_type=jnp.float32)
        row_max = jnp.max(logits, axis=-1, keepdims=True)
        exp_logits = jnp.exp(logits - row_max)
        row_sum = jnp.sum(exp_logits, axis=-1, keepdims=True)
        log_norm = row_max[:, 0] + jnp.log(row_sum[:, 0])
        is_target = col_ids == tgt_blk[:, None]
        tgt_logit = jnp.sum(jnp.where(is_target, logits, 0.0), axis=-1)
        loss_acc = loss_acc + jnp.sum(wt_blk * (log_norm - tgt_logit))
        d_logits = ((exp_logits / row_sum - is_target.astype(jnp.float32)) * wt_blk[:, None]).astype(jnp.bfloat16)
        d_normed = jnp.dot(d_logits, w_head.T, preferred_element_type=jnp.float32)
        d_x, d_scale = norm_vjp(d_normed)
        dw_acc = dw_acc + jnp.dot(normed.T, d_logits, preferred_element_type=jnp.float32)
        return (loss_acc, dscale_acc + d_scale, dw_acc), d_x.astype(jnp.bfloat16)

    init_carry = (jnp.zeros((), jnp.float32), jnp.zeros((MODEL_DIM,), jnp.float32), jnp.zeros((MODEL_DIM, VOCAB_PAD), jnp.float32))
    (total_loss, d_scale, d_w), d_x = lax.scan(block_step, init_carry, (x_blocks, tgt_blocks, tok_weight))
    return total_loss, d_x.reshape(BATCH, SEQ_LEN, MODEL_DIM), d_w, d_scale
```

```python
import functools

import jax
import jax.numpy as jnp
from jax import lax
from jax.experimental import pallas as pl
from jax.experimental.pallas import tpu as pltpu
from jax.sharding import PartitionSpec as P

EPS = 1e-5
BLK = 512
TN = 1024
CH = 128
GR = 16
KT = 1024
TN3 = 512
VB = 1024
BIG = 1e30
SOME = 1e29
LN = 128
LB = 9
LG = 4
LOG2E = 1.4426950408889634
LN2 = 0.6931471805599453
VMEM_MOST = 67043328
F32 = jnp.float32
BF16 = jnp.bfloat16
ANY = pl.BlockSpec(memory_space=pl.ANY)
SMEM = pl.BlockSpec(memory_space=pltpu.SMEM)


def mo(x, n):
    return pl.multiple_of(x, n)


def granules(sc, dev):
    return lax.shift_right_logical(sc[dev] + (GR - 1), LG)


def clip(x, lo, hi):
    return jnp.minimum(jnp.maximum(x, lo), hi)


def logits_kernel(c, first, last, n_dev, D, V, *refs):
    if first:
        sc, chunk, metab, w, z, nT, st, rem, mrem = refs[:9]
        rest = refs[9:]
    else:
        sc, chunk, metab, w = refs[:4]
        rem_in, mrem_in, z, nT, st, rem, mrem = refs[7:14]
        rest = refs[14:]
    nbuf, mbuf, stage, mstage, wbuf, zout, tbuf, mst, sst, tst, strow, qs, offs, semA, semS, semW, semZ, semT, semO = rest
    NT = V // TN
    HN = TN // 2
    RB = nbuf.shape[0]
    per = CH // GR
    ns = stage.shape[0]
    base_col = sc[n_dev]
    prev = jnp.int32(0)
    for g in range(n_dev):
        prev = prev + jnp.minimum(granules(sc, g), c * per)
    start = prev * GR
    r0 = start & (BLK - 1)
    base = lax.shift_right_logical(start, LB)
    tot = r0
    for g in range(n_dev):
        qg = clip(granules(sc, g) - c * per, 0, per)
        qs[g] = qg
        offs[g] = tot
        tot = tot + qg * GR
    nblk = lax.shift_right_logical(tot + (BLK - 1 if last else 0), LB)

    def wcopy(ct, slot):
        return pltpu.make_async_copy(w.at[:, pl.ds(mo(ct * TN, TN), TN)], wbuf.at[slot], semW.at[slot])

    @pl.when(nblk > 0)
    def _():
        wcopy(0, 0).start()

    mcp = pltpu.make_async_copy(metab.at[:, pl.ds(c * CH, CH), :], mstage, semA.at[0])
    mcp.start()
    head = pl.ds(0, BLK)
    if not first:
        rcp = pltpu.make_async_copy(rem_in, nbuf.at[head, :], semA.at[1])
        rcp.start()
        rmc = pltpu.make_async_copy(mrem_in, mbuf.at[head, :], semA.at[2])
        rmc.start()

    def scopy(g):
        k = g & (ns - 1)
        return pltpu.make_async_copy(chunk.at[g], stage.at[k], semS.at[k])

    for g in range(ns):
        scopy(g).start()
    if not first:
        rcp.wait()
        rmc.wait()
    mcp.wait()

    def convert(g):
        k = g & (ns - 1)
        scopy(g).wait()
        o = offs[g]

        def put(i):
            dst = pl.ds(mo(o + i * GR, GR), GR)
            src = pl.ds(mo(i * GR, GR), GR)
            nbuf[dst, :] = stage[k, src, :].astype(BF16)
            mbuf[dst, :] = mstage[g, src, :]

        @pl.when(qs[g] == per)
        def _():
            for i in range(per):
                put(i)

        @pl.when(qs[g] != per)
        def _():
            pl.loop(0, qs[g])(put)

        @pl.when(g + ns < n_dev)
        def _():
            scopy(g + ns).start()
        return g + 1

    def convert_to(g, row):
        return lax.while_loop(lambda g: (g < n_dev) & (offs[jnp.minimum(g, n_dev - 1)] < row), convert, g)

    if last:
        @pl.loop(0, lax.shift_right_logical(nblk * BLK - tot, LG))
        def _(i):
            dst = pl.ds(mo(tot + i * GR, GR), GR)
            nbuf[dst, :] = jnp.zeros((GR, D), BF16)
            mbuf[dst, :] = jnp.full((GR, LN), -1.0, F32)

    mst[...] = jnp.full_like(mst, -BIG)
    sst[...] = jnp.zeros_like(sst)
    tst[...] = jnp.zeros_like(tst)
    lane = lax.broadcasted_iota(jnp.int32, (1, LN), 1).astype(F32)
    colf = base_col.astype(F32)
    NH = BLK // LN

    def zcopy(slot, r, ct):
        cols = pl.ds(mo(ct * TN, TN), TN)
        return pltpu.make_async_copy(zout.at[slot], z.at[pl.ds(mo((base + r) * BLK, BLK), BLK), cols], semZ.at[slot])

    def tcopy(r):
        return pltpu.make_async_copy(tbuf, nT.at[:, pl.ds(mo((base + r) * BLK, BLK), BLK)], semT)

    HP = LN

    def epilogue(zq, x0, c0, h):
        rows = pl.ds(mo(x0 + h * HP, LN), HP)
        zh = zq[h * HP:(h + 1) * HP, :]
        m_old = mst[rows, :]
        m_new = m_old
        for j in range(HN // 2 // LN):
            m_new = jnp.maximum(m_new, zh[:, j * LN:(j + 1) * LN])
        s = sst[rows, :] * jnp.exp2(m_old - m_new)
        t = tst[rows, :]
        trel = mbuf[rows, :] - (lane + c0)
        for j in range(HN // 2 // LN):
            zz = zh[:, j * LN:(j + 1) * LN]
            s = s + jnp.exp2(zz - m_new)
            t = jnp.where(trel == float(j * LN), zz, t)
        mst[rows, :] = m_new
        sst[rows, :] = s
        tst[rows, :] = t

    def tile(ct, r, wslot, with_t):
        i = ct * nblk + r
        x0 = mo(r * BLK, BLK)
        x = nbuf[pl.ds(x0, BLK), :]
        c0 = colf + (ct * TN).astype(F32)

        slot = i & 1

        @pl.when(i >= 2)
        def _():
            zcopy(slot, 0, 0).wait()
        if with_t:
            @pl.when(r >= 1)
            def _():
                tcopy(0).wait()
        for k in range(2):
            for q in range(2):
                o = k * HN + q * HN // 2
                zq = jnp.dot(x, wbuf[wslot, :, o:o + HN // 2], preferred_element_type=F32) * LOG2E
                zout[slot, :, o:o + HN // 2] = zq
                for h in range(NH):
                    epilogue(zq, x0, c0 + o, h)
                if with_t:
                    hs = D // 4
                    o = (2 * k + q) * hs
                    for h in range(NH):
                        part = nbuf[pl.ds(mo(x0 + h * LN, LN), LN), o:o + hs]
                        tbuf[o:o + hs, h * LN:(h + 1) * LN] = part.T
        zcopy(slot, r, ct).start()
        if with_t:
            tcopy(r).start()

    def ct_step(ct, wslot, with_t, carry):
        wcopy(ct, wslot).wait()

        @pl.when(ct + 1 < NT)
        def _():
            wcopy(ct + 1, 1 - wslot).start()

        def rb(r, g):
            if with_t:
                g = convert_to(g, (r + 1) * BLK)
            tile(ct, r, wslot, with_t)
            return g

        return lax.fori_loop(0, nblk, rb, carry)

    @pl.when(nblk > 0)
    def _():
        convert_to(ct_step(jnp.int32(0), 0, True, jnp.int32(0)), tot + 1)

        def more(ct, carry):
            return ct_step(ct, ct & 1, False, carry)

        lax.fori_loop(1, NT, more, jnp.int32(0))

        @pl.loop(0, nblk)
        def _(r):
            for h in range(NH):
                rows = pl.ds(mo(r * BLK + h * LN, LN), LN)
                m = mst[rows, :]
                mr = jnp.max(m, axis=1, keepdims=True)
                sr = jnp.sum(sst[rows, :] * jnp.exp2(m - mr), axis=1, keepdims=True)
                tr = jnp.sum(tst[rows, :], axis=1, keepdims=True)
                tg = mbuf[rows, 0:1]
                bad = tg < 0.0
                mr = jnp.where(bad, BIG, mr)
                sr = jnp.where(bad, 1.0, sr)
                pack = jnp.where(lane == 0.0, mr, jnp.where(lane == 1.0, sr, jnp.where(lane == 2.0, tr, tg)))
                strow[:, pl.ds(mo(r * BLK + h * LN, LN), LN)] = pack.T[0:8, :]
            cols = pl.ds(mo((base + r) * BLK, BLK), BLK)
            pltpu.make_async_copy(strow.at[:, pl.ds(mo(r * BLK, BLK), BLK)], st.at[:, cols], semO.at[0]).start()

        @pl.loop(0, nblk)
        def _(r):
            pltpu.make_async_copy(strow.at[:, head], st.at[:, head], semO.at[0]).wait()
        zcopy(0, 0, 0).wait()
        zcopy(1, 0, 0).wait()
        tcopy(0).wait()

    @pl.when(nblk == 0)
    def _():
        convert_to(jnp.int32(0), tot + 1)

    rows = head if last else pl.ds(mo(nblk * BLK, BLK), BLK)
    a = pltpu.make_async_copy(nbuf.at[rows, :], rem, semO.at[1])
    b = pltpu.make_async_copy(mbuf.at[rows, :], mrem, semO.at[2])
    a.start()
    b.start()
    a.wait()
    b.wait()


def logits_call(c, first, last, n_dev, D, V, R, sc, chunk, metab, w, state):
    RB = BLK + n_dev * CH
    out_shape = [
        jax.ShapeDtypeStruct((R + BLK, V), F32),
        jax.ShapeDtypeStruct((D, R), BF16),
        jax.ShapeDtypeStruct((8, R), F32),
        jax.ShapeDtypeStruct((BLK, D), BF16),
        jax.ShapeDtypeStruct((BLK, LN), F32),
    ]
    ins = [sc, chunk, metab, w] + ([] if first else list(state))
    dma = pltpu.SemaphoreType.DMA
    return pl.pallas_call(
        functools.partial(logits_kernel, c, first, last, n_dev, D, V),
        grid_spec=pltpu.PrefetchScalarGridSpec(
            num_scalar_prefetch=1,
            grid=(1,),
            in_specs=[ANY] * (len(ins) - 1),
            out_specs=[ANY] * len(out_shape),
            scratch_shapes=[
                pltpu.VMEM((RB, D), BF16),
                pltpu.VMEM((RB, LN), F32),
                pltpu.VMEM((4, CH, D), F32),
                pltpu.VMEM((n_dev, CH, LN), F32),
                pltpu.VMEM((2, D, TN), BF16),
                pltpu.VMEM((2, BLK, TN), F32),
                pltpu.VMEM((D, BLK), BF16),
                pltpu.VMEM((RB, LN), F32),
                pltpu.VMEM((RB, LN), F32),
                pltpu.VMEM((RB, LN), F32),
                pltpu.VMEM((8, RB), F32),
                pltpu.SMEM((n_dev,), jnp.int32),
                pltpu.SMEM((n_dev,), jnp.int32),
                dma((3,)), dma((4,)), dma((2,)), dma((2,)), dma, dma((3,)),
            ],
        ),
        out_shape=out_shape,
        input_output_aliases={} if first else {4 + i: i for i in range(3)},
        compiler_params=pltpu.CompilerParams(vmem_limit_bytes=VMEM_MOST),
        cost_estimate=pl.CostEstimate(flops=n_dev * CH * D * V, bytes_accessed=D * V * 2, transcendentals=0),
        name=f"logits{c}",
    )(*ins)


def stats_kernel(nr, n_dev, n_vp, sc, fs, st, L, T, loss, stv, buf, sem, send, recv):
    me = lax.axis_index("vp")
    barrier = pltpu.get_barrier_semaphore()
    cp = pltpu.make_async_copy(st.at[:, pl.ds(0, nr * LN)], stv, sem)
    cp.start()
    for d in range(1, n_vp):
        pl.semaphore_signal(barrier, inc=1, device_id={"vp": lax.rem(me + d, n_vp)}, device_id_type=pl.DeviceIdType.MESH)
    n16 = jnp.int32(0)
    for g in range(n_dev):
        n16 = n16 + granules(sc, g) * GR
    cp.wait()
    lane = lax.broadcasted_iota(jnp.int32, (1, LN), 1)
    live = lax.broadcasted_iota(jnp.int32, (nr, LN), 0) * LN + lax.broadcasted_iota(jnp.int32, (nr, LN), 1) < n16
    tz = jnp.zeros((1, LN), F32)
    for i in range(nr):
        cols = slice(i * LN, (i + 1) * LN)
        mi = stv[0:1, cols]
        buf[me, i:i + 1, :] = mi
        buf[me, nr + i:nr + i + 1, :] = stv[1:2, cols]
        T[i:i + 1, :] = stv[3:4, cols]
        tz = tz + jnp.where((lane + i * LN < n16) & (mi < SOME), stv[2:3, cols], 0.0)
    buf[me, 2 * nr:2 * nr + 8, :] = jnp.broadcast_to(tz, (8, LN))
    pl.semaphore_wait(barrier, n_vp - 1)
    copies = []
    for d in range(n_vp - 1):
        copies.append(pltpu.make_async_remote_copy(
            src_ref=buf.at[me], dst_ref=buf.at[me], send_sem=send.at[d], recv_sem=recv.at[d],
            device_id={"vp": lax.rem(me + d + 1, n_vp)}, device_id_type=pl.DeviceIdType.MESH))
    for c in copies:
        c.start()
    for c in copies:
        c.wait()
    m = buf[0, 0:nr, :]
    for p in range(1, n_vp):
        m = jnp.maximum(m, buf[p, 0:nr, :])
    s = jnp.zeros((nr, LN), F32)
    tz = jnp.zeros((1, LN), F32)
    for p in range(n_vp):
        s = s + buf[p, nr:2 * nr, :] * jnp.exp2(buf[p, 0:nr, :] - m)
        tz = tz + buf[p, 2 * nr:2 * nr + 1, :]
    lse = m + jnp.log(s) * LOG2E
    total = jnp.sum(jnp.where(live & (m < SOME), lse, 0.0)) - jnp.sum(tz)
    loss[...] = jnp.full((8, LN), total * (fs[0] * LN2), F32)
    L[0:nr, :] = lse + fs[1]


def stats_call(nr, n_dev, n_vp, R, cid, sc, fs, st):
    vm = pl.BlockSpec(memory_space=pltpu.VMEM)
    rows = jax.ShapeDtypeStruct((R // LN + 8, LN), F32)
    return pl.pallas_call(
        functools.partial(stats_kernel, nr, n_dev, n_vp),
        in_specs=[SMEM, SMEM, ANY],
        out_specs=[vm, vm, vm],
        out_shape=[rows, rows, jax.ShapeDtypeStruct((8, LN), F32)],
        scratch_shapes=[
            pltpu.VMEM((8, nr * LN), F32),
            pltpu.VMEM((n_vp, 2 * nr + 8, LN), F32),
            pltpu.SemaphoreType.DMA,
            pltpu.SemaphoreType.DMA((n_vp - 1,)),
            pltpu.SemaphoreType.DMA((n_vp - 1,)),
        ],
        compiler_params=pltpu.CompilerParams(collective_id=cid, has_side_effects=True, vmem_limit_bytes=VMEM_MOST // 2),
        name=f"stats{nr}",
    )(sc, fs, st)


def make_dz(zb, lt, i0, c0, lane, w, dst, jobs):
    for r, j in jobs:
        rs = slice(r * LN, (r + 1) * LN)
        cs = slice(j * LN, (j + 1) * LN)
        lr = jnp.broadcast_to(lt[0][pl.ds(i0 + r, 1), :], (LN, LN)).T
        trel = jnp.broadcast_to(lt[1][pl.ds(i0 + r, 1), :], (LN, LN)).T - (lane + c0)
        p = jnp.exp2(zb[rs, cs] - lr)
        dst[rs, cs] = (p - jnp.where(trel == float(j * LN), w, 0.0)).astype(BF16)


def dn_kernel(nch, n_dev, n_vp, D, V, sc, fs, L, T, z, w_hbm, dn, wb, zA, zB, dzA, dzB, acc, bsrc, brow, bgr, bcnt, dst, wsem, zsem, osem):
    NV = V // VB
    per = CH // GR
    C = nch * CH
    w = fs[0]
    colf = sc[n_dev].astype(F32)
    dp = sc[n_dev + 1]
    lane = lax.broadcasted_iota(jnp.int32, (1, LN), 1).astype(F32)
    lt = (L, T)

    def wcopy(v):
        cols = pl.ds(mo(v * VB, VB), VB)
        return pltpu.make_async_copy(w_hbm.at[:, cols], wb.at[:, cols], wsem.at[v])

    wcopy(0).start()
    pos = jnp.int32(0)
    nblk = jnp.int32(0)
    n = jnp.int32(0)
    for c in range(nch):
        start = pos
        mine = jnp.int32(0)
        for g in range(n_dev):
            qg = clip(granules(sc, g) - c * per, 0, per)
            pos = pos + qg * GR
            start = start + jnp.where(g // n_vp < dp, qg * GR, 0)
            mine = mine + jnp.where(g // n_vp == dp, qg, 0)
        end = start + mine * GR
        low = start & -LN
        cnt = jnp.where(mine > 0, lax.shift_right_logical(end - low + BLK - 1, LB), 0)

        def fill(i, n, c=c, start=start, end=end, low=low, nblk=nblk):
            src = low + i * BLK
            lo = jnp.maximum(src, start)
            ng = lax.shift_right_logical(jnp.minimum(src + BLK, end) - lo, LG)
            bsrc[nblk + i] = src
            brow[nblk + i] = lo - src
            bgr[nblk + i] = n
            bcnt[nblk + i] = ng
            return n + ng

        n0 = n
        n = lax.fori_loop(0, cnt, fill, n)
        nblk = nblk + cnt
        for e in range(n_vp):
            qe = clip(granules(sc, dp * n_vp + e) - c * per, 0, per)

            @pl.loop(0, qe)
            def _(i, c=c, e=e, n0=n0):
                dst[n0 + i] = e * C + c * CH + i * GR
            n0 = n0 + qe

    def zcopy(b, vb, k):
        rows = pl.ds(mo(bsrc[b], LN), BLK)
        return pltpu.make_async_copy(z.at[rows, pl.ds(mo(vb * VB, VB), VB)], (zA, zB)[k], zsem.at[k])

    def ocopy(s, a, r):
        return pltpu.make_async_copy(acc.at[s, pl.ds(mo(a, GR), GR), :], dn.at[pl.ds(mo(r, GR), GR), :], osem.at[s])

    def ostart(b, s):
        @pl.loop(0, bcnt[b])
        def _(i):
            ocopy(s, brow[b] + i * GR, dst[bgr[b] + i]).start()

    def owait(b, s):
        @pl.loop(0, bcnt[b])
        def _(i):
            ocopy(s, 0, 0).wait()

    NR = BLK // LN
    NC = D // 512

    @pl.when(nblk == 0)
    def _():
        wcopy(0).wait()

    @pl.when(nblk > 0)
    def _():
        zcopy(0, 0, 0).start()
        zcopy(0, 1, 1).start()
        for v in range(1, NV):
            wcopy(v).start()
        zcopy(0, 0, 0).wait()
        everything = [(r, j) for r in range(NR) for j in range(VB // LN)]
        make_dz(zA, lt, lax.shift_right_logical(bsrc[0], LB - 2), colf, lane, w, dzA, everything)
        step = -(-len(everything) // (NC - 1))

        def half(b, vb, wraps, cur, nxt, k):
            s = b & 1
            first = vb == 0
            nb = jnp.minimum(b + jnp.where(wraps, 1, 0), nblk - 1)
            nvb = jnp.where(wraps, 0, vb + 1)

            @pl.when(jnp.logical_not(wraps) | (b + 1 < nblk))
            def _():
                zcopy(0, 0, k).wait()
            v2 = vb + 2
            over = v2 >= NV
            b2 = b + jnp.where(over, 1, 0)

            @pl.when(b2 < nblk)
            def _():
                zcopy(b2, jnp.where(over, v2 - NV, v2), 1 - k).start()

            @pl.when(first & (b >= 2))
            def _():
                owait(b - 2, s)

            @pl.when(b == 0)
            def _():
                wcopy(vb).wait()
            c0 = colf + (nvb * VB).astype(F32)
            i0 = lax.shift_right_logical(bsrc[nb], LB - 2)

            def run(rows):
                for q in range(NC):
                    cs = slice(q * 512, (q + 1) * 512)
                    y = lax.dot_general(cur[0:rows, :], wb[cs, pl.ds(mo(vb * VB, VB), VB)], (((1,), (1,)), ((), ())), preferred_element_type=F32)
                    acc[s, 0:rows, cs] = jnp.where(first, 0.0, acc[s, 0:rows, cs]) + y
                    make_dz((zA, zB)[k], lt, i0, c0, lane, w, nxt, everything[q * step:(q + 1) * step])

            small = brow[b] + bcnt[b] * GR <= BLK // 2

            @pl.when(small)
            def _():
                run(BLK // 2)

            @pl.when(jnp.logical_not(small))
            def _():
                run(BLK)

            @pl.when(wraps)
            def _():
                ostart(b, s)

        @pl.loop(0, nblk)
        def _(b):
            @pl.loop(0, NV // 2)
            def _(v):
                half(b, 2 * v, jnp.bool_(False), dzA, dzB, 1)
                half(b, 2 * v + 1, v == NV // 2 - 1, dzB, dzA, 0)

        @pl.when(nblk >= 2)
        def _():
            owait(nblk - 2, nblk & 1)
        owait(nblk - 1, (nblk - 1) & 1)


def dn_call(nch, n_dev, n_vp, D, V, sc, fs, L, T, z, w):
    dma = pltpu.SemaphoreType.DMA
    vm = pl.BlockSpec(memory_space=pltpu.VMEM)
    table = pltpu.SMEM((64,), jnp.int32)
    return pl.pallas_call(
        functools.partial(dn_kernel, nch, n_dev, n_vp, D, V),
        in_specs=[SMEM, SMEM, vm, vm, ANY, ANY],
        out_specs=ANY,
        out_shape=jax.ShapeDtypeStruct((n_vp * nch * CH, D), F32),
        scratch_shapes=[
            pltpu.VMEM((D, V), BF16),
            pltpu.VMEM((BLK, VB), F32),
            pltpu.VMEM((BLK, VB), F32),
            pltpu.VMEM((BLK, VB), BF16),
            pltpu.VMEM((BLK, VB), BF16),
            pltpu.VMEM((2, BLK, D), F32),
            table, table, table, table,
            pltpu.SMEM((n_vp * nch * CH // GR,), jnp.int32),
            dma((V // VB,)), dma((2,)), dma((2,)),
        ],
        compiler_params=pltpu.CompilerParams(vmem_limit_bytes=VMEM_MOST),
        cost_estimate=pl.CostEstimate(flops=n_vp * nch * CH * D * V, bytes_accessed=D * V * 2, transcendentals=0),
        name=f"dn{nch}",
    )(sc, fs, L, T, z, w)


def dw_kernel(n_dev, D, V, sc, fs, L, T, nT, z, dw, nb, zA, zB, dzA, dzB, acc, nsem, zsem, osem):
    NT = V // TN3
    w = fs[0]
    colf = sc[n_dev].astype(F32)
    lane = lax.broadcasted_iota(jnp.int32, (1, LN), 1).astype(F32)
    lt = (L, T)
    g16 = jnp.int32(0)
    for g in range(n_dev):
        g16 = g16 + granules(sc, g)
    nb512 = lax.shift_right_logical(g16 * GR + BLK - 1, LB)
    S = lax.shift_right_logical(nb512 + 1, 1)
    odd = nb512 & 1
    NR = KT // LN

    def ncopy(t):
        cols = pl.ds(mo(t * BLK, BLK), BLK)
        return pltpu.make_async_copy(nT.at[:, cols], nb.at[:, cols], nsem.at[t])

    def is_half(t):
        return (t == S - 1) & (odd == 1)

    def zgo(ct, t, k, start):
        h = is_half(t)
        for size, cond in ((KT, jnp.logical_not(h)), (BLK, h)):
            @pl.when(cond)
            def _(size=size):
                cols = pl.ds(mo(ct * TN3, TN3), TN3)
                c = pltpu.make_async_copy(z.at[pl.ds(mo(t * KT, KT), size), cols], (zA, zB)[k].at[pl.ds(0, size), :], zsem.at[k])
                if start:
                    c.start()
                else:
                    c.wait()

    def nxt(ct, t):
        wrap = t + 1 == S
        return ct + jnp.where(wrap, 1, 0), jnp.where(wrap, 0, t + 1)

    def ocopy(ct, s):
        return pltpu.make_async_copy(acc.at[s], dw.at[:, pl.ds(mo(ct * TN3, TN3), TN3)], osem.at[s])

    MS = 512
    NM = D // MS
    zero = jnp.int32(0)
    zgo(zero, zero, 0, True)
    c1, t1 = nxt(zero, zero)
    zgo(c1, t1, 1, True)

    @pl.loop(0, nb512)
    def _(t):
        ncopy(t).start()
    zgo(zero, zero, 0, False)
    jobs = [(r, j) for r in range(NR) for j in range(TN3 // LN)]
    make_dz(zA, lt, zero, colf, lane, w, dzA, jobs)
    step = -(-len(jobs) // (NM - 1))
    c2, t2 = nxt(c1, t1)
    zgo(c2, t2, 0, True)

    def half(ct, t, cur, nxtbuf, k):
        s = ct & 1
        na, ta = nxt(ct, t)
        nb_, tb_ = nxt(na, ta)
        nc, tc = nxt(nb_, tb_)

        @pl.when(na < NT)
        def _():
            zgo(na, ta, k, False)

        @pl.when(ct == 0)
        def _():
            ncopy(2 * t).wait()

            @pl.when(jnp.logical_not(is_half(t)))
            def _():
                ncopy(2 * t + 1).wait()

        @pl.when((t == 0) & (ct >= 2))
        def _():
            ocopy(0, s).wait()
        c0 = colf + (na * TN3).astype(F32)
        i0 = ta * NR
        first = t == 0

        def run(size):
            cols = pl.ds(mo(t * KT, KT), size)
            for m in range(NM):
                ms = slice(m * MS, (m + 1) * MS)
                y = jnp.dot(nb[ms, cols], cur[0:size, :], preferred_element_type=F32)
                acc[s, ms, :] = jnp.where(first, 0.0, acc[s, ms, :]) + y
                make_dz((zA, zB)[k], lt, i0, c0, lane, w, nxtbuf, jobs[m * step:(m + 1) * step])

        h = is_half(t)

        @pl.when(jnp.logical_not(h))
        def _():
            run(KT)

        @pl.when(h)
        def _():
            run(BLK)

        @pl.when(nc < NT)
        def _():
            zgo(nc, tc, k, True)

        @pl.when(t == S - 1)
        def _():
            ocopy(ct, s).start()
        return na, ta

    def pair(i, carry):
        ct, t = carry
        ct, t = half(ct, t, dzA, dzB, 1)
        return half(ct, t, dzB, dzA, 0)

    lax.fori_loop(0, S * (NT // 2), pair, (zero, zero))
    ocopy(0, 0).wait()
    ocopy(0, 1).wait()


def dw_call(n_dev, D, V, R, rows_est, sc, fs, L, T, nT, z):
    dma = pltpu.SemaphoreType.DMA
    vm = pl.BlockSpec(memory_space=pltpu.VMEM)
    return pl.pallas_call(
        functools.partial(dw_kernel, n_dev, D, V),
        in_specs=[SMEM, SMEM, vm, vm, ANY, ANY],
        out_specs=ANY,
        out_shape=jax.ShapeDtypeStruct((D, V), F32),
        scratch_shapes=[
            pltpu.VMEM((D, R), BF16),
            pltpu.VMEM((KT, TN3), F32),
            pltpu.VMEM((KT, TN3), F32),
            pltpu.VMEM((KT, TN3), BF16),
            pltpu.VMEM((KT, TN3), BF16),
            pltpu.VMEM((2, D, TN3), F32),
            dma((R // BLK,)), dma((2,)), dma((2,)),
        ],
        compiler_params=pltpu.CompilerParams(vmem_limit_bytes=VMEM_MOST),
        cost_estimate=pl.CostEstimate(flops=2 * rows_est * D * V, bytes_accessed=D * V * 4, transcendentals=0),
        name="dw",
    )(sc, fs, L, T, nT, z)


def solution(mesh):
    n_vp = mesh.shape["vp"]
    n_dp = mesh.shape["dp"]
    n_dev = n_vp * n_dp

    def local_step(hidden, targets, loss_mask, norm_scale, w_head):
        D, V = w_head.shape
        tok = hidden.shape[1]
        R = n_dev * tok
        x = hidden[0]
        x_f32 = x.astype(F32)
        inv_rms = lax.rsqrt(jnp.mean(x_f32 * x_f32, axis=-1, keepdims=True) + EPS)
        normed = (x_f32 * inv_rms * norm_scale).astype(BF16)
        keep = loss_mask[0] > 0
        keep_b = keep.astype(BF16)
        before = (lax.broadcasted_iota(jnp.int32, (tok, tok), 1) >= lax.broadcasted_iota(jnp.int32, (tok, tok), 0)).astype(BF16)
        rank = jnp.dot(keep_b[None, :], before, preferred_element_type=F32)[0].astype(jnp.int32) - 1
        slot = lax.broadcasted_iota(jnp.int32, (tok, tok), 0)
        perm = ((slot == rank[None, :]) & keep[None, :]).astype(BF16)
        sent = jnp.dot(perm, normed, preferred_element_type=F32)
        tgt = targets[0]
        pair = jnp.stack([(tgt // 256).astype(BF16), (tgt % 256).astype(BF16), keep_b], axis=1)
        got = jnp.dot(perm, pair, preferred_element_type=F32)
        meta = jnp.where(got[:, 2] > 0.5, got[:, 0] * 256.0 + got[:, 1], -1.0)

        def gather(c):
            return lax.all_gather(sent[c * CH:(c + 1) * CH], ("dp", "vp"), axis=0, tiled=False)

        chunk0 = gather(0)
        metas = lax.all_gather(meta, ("dp", "vp"), axis=0, tiled=False)
        counts = jnp.sum((metas >= 0.0).astype(jnp.int32), axis=1)
        count = jnp.sum(counts).astype(F32)
        weight = 1.0 / count
        sc = jnp.concatenate([counts, jnp.stack([lax.axis_index("vp") * V, lax.axis_index("dp")])]).astype(jnp.int32)
        fs = jnp.stack([weight, jnp.log(count) * LOG2E])
        metab = jnp.broadcast_to(metas[:, :, None], (n_dev, tok, LN))
        most = jnp.max(counts)
        branch = clip((most + (CH - 1)) // CH - 1, 0, tok // CH - 1)

        def make(nch):
            def run(chunk0, sent, metab, sc, fs, w_head, x, perm, norm_scale, meta):
                chunks = [chunk0] + [
                    lax.all_gather(sent[c * CH:(c + 1) * CH], ("dp", "vp"), axis=0, tiled=False) for c in range(1, nch)
                ]
                state = None
                for c in range(nch):
                    state = logits_call(c, c == 0, c == nch - 1, n_dev, D, V, R, sc, chunks[c], metab, w_head, state)
                z, nT, st = state[:3]
                L, T, loss = stats_call(nch * CH * n_dev // LN, n_dev, n_vp, R, nch, sc, fs, st)
                dn = dn_call(nch, n_dev, n_vp, D, V, sc, fs, L, T, z, w_head)
                C = nch * CH
                d_normed = lax.psum_scatter(dn, "vp", scatter_dimension=0, tiled=True)
                d_w = dw_call(n_dev, D, V, R, n_dev * C // 2, sc, fs, L, T, nT, z)
                xc = jnp.dot(perm[:C], x, preferred_element_type=F32)
                live = (meta[:C] >= 0.0)[:, None]
                rc = lax.rsqrt(jnp.mean(xc * xc, axis=-1, keepdims=True) + EPS)
                xh = xc * rc
                d_normed = jnp.where(live, d_normed, 0.0)
                d_scale = jnp.sum(d_normed * xh, axis=0)
                e = d_normed * norm_scale
                dx = rc * (e - xh * jnp.mean(e * xh, axis=-1, keepdims=True))
                d_hidden = lax.dot_general(perm[:C], dx.astype(BF16), (((0,), (0,)), ((), ())), preferred_element_type=F32).astype(BF16)
                d_scale = lax.psum(d_scale, ("dp", "vp"))
                return loss[0, 0], d_hidden, d_w, d_scale
            return run

        loss, d_hidden, d_w, d_scale = lax.switch(
            branch, [make(i + 1) for i in range(tok // CH)],
            chunk0, sent, metab, sc, fs, w_head, x, perm, norm_scale, meta)
        return loss, d_hidden[None], d_w, d_scale

    return jax.shard_map(
        local_step,
        mesh=mesh,
        in_specs=(P("dp", "vp", None), P("dp", "vp"), P("dp", "vp"), P(None), P(None, "vp")),
        out_specs=(P(), P("dp", "vp", None), P(None, "vp"), P(None)),
        check_vma=False,
    )
```

```python
import functools

import jax
import jax.numpy as jnp
from jax import lax
from jax.experimental import pallas as pl
from jax.experimental.pallas import tpu as pltpu
from jax.sharding import PartitionSpec as P

EPS = 1e-5
BLK = 512
TN = 1024
CHS = (64, 96, 128, 128, 96)
GR = 16
KT = 1024
TN3 = 512
VB = 1024
BIG = 1e30
SOME = 1e29
LN = 128
LB = 9
LG = 4
LOG2E = 1.4426950408889634
LN2 = 0.6931471805599453
VMEM_MOST = 67043328
F32 = jnp.float32
BF16 = jnp.bfloat16
ANY = pl.BlockSpec(memory_space=pl.ANY)
SMEM = pl.BlockSpec(memory_space=pltpu.SMEM)


def mo(x, n):
    return pl.multiple_of(x, n)


def granules(sc, dev):
    return lax.shift_right_logical(sc[dev] + (GR - 1), LG)


def clip(x, lo, hi):
    return jnp.minimum(jnp.maximum(x, lo), hi)


def logits_kernel(c, first, last, n_dev, D, V, *refs):
    if first:
        sc, chunk, metab, w, z, nT, st, rem, mrem = refs[:9]
        rest = refs[9:]
    else:
        sc, chunk, metab, w = refs[:4]
        rem_in, mrem_in, z, nT, st, rem, mrem = refs[7:14]
        rest = refs[14:]
    nbuf, mbuf, stage, mstage, wbuf, zout, tbuf, mst, sst, tst, strow, qs, offs, semA, semS, semW, semZ, semT, semO = rest
    NT = V // TN
    HN = TN // 2
    RB = nbuf.shape[0]
    per = CHS[c] // GR
    g0 = sum(CHS[:c]) // GR
    ns = stage.shape[0]
    base_col = sc[n_dev]
    prev = jnp.int32(0)
    for g in range(n_dev):
        prev = prev + jnp.minimum(granules(sc, g), g0)
    start = prev * GR
    r0 = start & (BLK - 1)
    base = lax.shift_right_logical(start, LB)
    tot = r0
    for g in range(n_dev):
        qg = clip(granules(sc, g) - g0, 0, per)
        qs[g] = qg
        offs[g] = tot
        tot = tot + qg * GR
    nblk = lax.shift_right_logical(tot + (BLK - 1 if last else 0), LB)

    def wcopy(ct, slot):
        return pltpu.make_async_copy(w.at[:, pl.ds(mo(ct * TN, TN), TN)], wbuf.at[slot], semW.at[slot])

    @pl.when(nblk > 0)
    def _():
        wcopy(0, 0).start()

    mcp = pltpu.make_async_copy(metab.at[:, pl.ds(g0 * GR, per * GR), :], mstage, semA.at[0])
    mcp.start()
    head = pl.ds(0, BLK)
    if not first:
        rcp = pltpu.make_async_copy(rem_in, nbuf.at[head, :], semA.at[1])
        rcp.start()
        rmc = pltpu.make_async_copy(mrem_in, mbuf.at[head, :], semA.at[2])
        rmc.start()

    def scopy(g):
        k = g & (ns - 1)
        return pltpu.make_async_copy(chunk.at[g], stage.at[k], semS.at[k])

    for g in range(ns):
        scopy(g).start()
    if not first:
        rcp.wait()
        rmc.wait()
    mcp.wait()

    def convert(g):
        k = g & (ns - 1)
        scopy(g).wait()
        o = offs[g]

        def put(i):
            dst = pl.ds(mo(o + i * GR, GR), GR)
            src = pl.ds(mo(i * GR, GR), GR)
            nbuf[dst, :] = stage[k, src, :].astype(BF16)
            mbuf[dst, :] = mstage[g, src, :]

        @pl.when(qs[g] == per)
        def _():
            for i in range(per):
                put(i)

        @pl.when(qs[g] != per)
        def _():
            pl.loop(0, qs[g])(put)

        @pl.when(g + ns < n_dev)
        def _():
            scopy(g + ns).start()
        return g + 1

    def convert_to(g, row):
        return lax.while_loop(lambda g: (g < n_dev) & (offs[jnp.minimum(g, n_dev - 1)] < row), convert, g)

    if last:
        @pl.loop(0, lax.shift_right_logical(nblk * BLK - tot, LG))
        def _(i):
            dst = pl.ds(mo(tot + i * GR, GR), GR)
            nbuf[dst, :] = jnp.zeros((GR, D), BF16)
            mbuf[dst, :] = jnp.full((GR, LN), -1.0, F32)

    mst[...] = jnp.full_like(mst, -BIG)
    sst[...] = jnp.zeros_like(sst)
    tst[...] = jnp.zeros_like(tst)
    lane = lax.broadcasted_iota(jnp.int32, (1, LN), 1).astype(F32)
    colf = base_col.astype(F32)
    NH = BLK // LN

    def zcopy(slot, r, ct):
        cols = pl.ds(mo(ct * TN, TN), TN)
        return pltpu.make_async_copy(zout.at[slot], z.at[pl.ds(mo((base + r) * BLK, BLK), BLK), cols], semZ.at[slot])

    def tcopy(r):
        return pltpu.make_async_copy(tbuf, nT.at[:, pl.ds(mo((base + r) * BLK, BLK), BLK)], semT)

    HP = LN

    def epilogue(zq, x0, c0, h):
        rows = pl.ds(mo(x0 + h * HP, LN), HP)
        zh = zq[h * HP:(h + 1) * HP, :]
        m_old = mst[rows, :]
        m_new = m_old
        for j in range(HN // 2 // LN):
            m_new = jnp.maximum(m_new, zh[:, j * LN:(j + 1) * LN])
        s = sst[rows, :] * jnp.exp2(m_old - m_new)
        t = tst[rows, :]
        trel = mbuf[rows, :] - (lane + c0)
        for j in range(HN // 2 // LN):
            zz = zh[:, j * LN:(j + 1) * LN]
            s = s + jnp.exp2(zz - m_new)
            t = jnp.where(trel == float(j * LN), zz, t)
        mst[rows, :] = m_new
        sst[rows, :] = s
        tst[rows, :] = t

    def tile(ct, r, wslot, with_t):
        i = ct * nblk + r
        x0 = mo(r * BLK, BLK)
        x = nbuf[pl.ds(x0, BLK), :]
        c0 = colf + (ct * TN).astype(F32)

        slot = i & 1

        @pl.when(i >= 2)
        def _():
            zcopy(slot, 0, 0).wait()
        if with_t:
            @pl.when(r >= 1)
            def _():
                tcopy(0).wait()
        for k in range(2):
            for q in range(2):
                o = k * HN + q * HN // 2
                zq = jnp.dot(x, wbuf[wslot, :, o:o + HN // 2], preferred_element_type=F32) * LOG2E
                zout[slot, :, o:o + HN // 2] = zq
                for h in range(NH):
                    epilogue(zq, x0, c0 + o, h)
                if with_t:
                    hs = D // 4
                    o = (2 * k + q) * hs
                    for h in range(NH):
                        part = nbuf[pl.ds(mo(x0 + h * LN, LN), LN), o:o + hs]
                        tbuf[o:o + hs, h * LN:(h + 1) * LN] = part.T
        zcopy(slot, r, ct).start()
        if with_t:
            tcopy(r).start()

    def ct_step(ct, wslot, with_t, carry):
        wcopy(ct, wslot).wait()

        @pl.when(ct + 1 < NT)
        def _():
            wcopy(ct + 1, 1 - wslot).start()

        def rb(r, g):
            if with_t:
                g = convert_to(g, (r + 1) * BLK)
            tile(ct, r, wslot, with_t)
            return g

        return lax.fori_loop(0, nblk, rb, carry)

    @pl.when(nblk > 0)
    def _():
        convert_to(ct_step(jnp.int32(0), 0, True, jnp.int32(0)), tot + 1)

        def more(ct, carry):
            return ct_step(ct, ct & 1, False, carry)

        lax.fori_loop(1, NT, more, jnp.int32(0))

        @pl.loop(0, nblk)
        def _(r):
            for h in range(NH):
                rows = pl.ds(mo(r * BLK + h * LN, LN), LN)
                m = mst[rows, :]
                mr = jnp.max(m, axis=1, keepdims=True)
                sr = jnp.sum(sst[rows, :] * jnp.exp2(m - mr), axis=1, keepdims=True)
                tr = jnp.sum(tst[rows, :], axis=1, keepdims=True)
                tg = mbuf[rows, 0:1]
                bad = tg < 0.0
                mr = jnp.where(bad, BIG, mr)
                sr = jnp.where(bad, 1.0, sr)
                pack = jnp.where(lane == 0.0, mr, jnp.where(lane == 1.0, sr, jnp.where(lane == 2.0, tr, tg)))
                strow[:, pl.ds(mo(r * BLK + h * LN, LN), LN)] = pack.T[0:8, :]
            cols = pl.ds(mo((base + r) * BLK, BLK), BLK)
            pltpu.make_async_copy(strow.at[:, pl.ds(mo(r * BLK, BLK), BLK)], st.at[:, cols], semO.at[0]).start()

        @pl.loop(0, nblk)
        def _(r):
            pltpu.make_async_copy(strow.at[:, head], st.at[:, head], semO.at[0]).wait()
        zcopy(0, 0, 0).wait()
        zcopy(1, 0, 0).wait()
        tcopy(0).wait()

    @pl.when(nblk == 0)
    def _():
        convert_to(jnp.int32(0), tot + 1)

    rows = head if last else pl.ds(mo(nblk * BLK, BLK), BLK)
    a = pltpu.make_async_copy(nbuf.at[rows, :], rem, semO.at[1])
    b = pltpu.make_async_copy(mbuf.at[rows, :], mrem, semO.at[2])
    a.start()
    b.start()
    a.wait()
    b.wait()


def logits_call(c, first, last, n_dev, D, V, R, sc, chunk, metab, w, state):
    RB = BLK + n_dev * CHS[c]
    out_shape = [
        jax.ShapeDtypeStruct((R + BLK, V), F32),
        jax.ShapeDtypeStruct((D, R), BF16),
        jax.ShapeDtypeStruct((8, R), F32),
        jax.ShapeDtypeStruct((BLK, D), BF16),
        jax.ShapeDtypeStruct((BLK, LN), F32),
    ]
    ins = [sc, chunk, metab, w] + ([] if first else list(state))
    dma = pltpu.SemaphoreType.DMA
    return pl.pallas_call(
        functools.partial(logits_kernel, c, first, last, n_dev, D, V),
        grid_spec=pltpu.PrefetchScalarGridSpec(
            num_scalar_prefetch=1,
            grid=(1,),
            in_specs=[ANY] * (len(ins) - 1),
            out_specs=[ANY] * len(out_shape),
            scratch_shapes=[
                pltpu.VMEM((RB, D), BF16),
                pltpu.VMEM((RB, LN), F32),
                pltpu.VMEM((4, CHS[c], D), F32),
                pltpu.VMEM((n_dev, CHS[c], LN), F32),
                pltpu.VMEM((2, D, TN), BF16),
                pltpu.VMEM((2, BLK, TN), F32),
                pltpu.VMEM((D, BLK), BF16),
                pltpu.VMEM((RB, LN), F32),
                pltpu.VMEM((RB, LN), F32),
                pltpu.VMEM((RB, LN), F32),
                pltpu.VMEM((8, RB), F32),
                pltpu.SMEM((n_dev,), jnp.int32),
                pltpu.SMEM((n_dev,), jnp.int32),
                dma((3,)), dma((4,)), dma((2,)), dma((2,)), dma, dma((3,)),
            ],
        ),
        out_shape=out_shape,
        input_output_aliases={} if first else {4 + i: i for i in range(3)},
        compiler_params=pltpu.CompilerParams(vmem_limit_bytes=VMEM_MOST),
        cost_estimate=pl.CostEstimate(flops=n_dev * CHS[c] * D * V, bytes_accessed=D * V * 2, transcendentals=0),
        name=f"logits{c}",
    )(*ins)


def stats_kernel(nr, n_dev, n_vp, sc, fs, st, L, T, loss, stv, buf, sem, send, recv):
    me = lax.axis_index("vp")
    barrier = pltpu.get_barrier_semaphore()
    cp = pltpu.make_async_copy(st.at[:, pl.ds(0, nr * LN)], stv, sem)
    cp.start()
    for d in range(1, n_vp):
        pl.semaphore_signal(barrier, inc=1, device_id={"vp": lax.rem(me + d, n_vp)}, device_id_type=pl.DeviceIdType.MESH)
    n16 = jnp.int32(0)
    for g in range(n_dev):
        n16 = n16 + granules(sc, g) * GR
    cp.wait()
    lane = lax.broadcasted_iota(jnp.int32, (1, LN), 1)
    live = lax.broadcasted_iota(jnp.int32, (nr, LN), 0) * LN + lax.broadcasted_iota(jnp.int32, (nr, LN), 1) < n16
    tz = jnp.zeros((1, LN), F32)
    for i in range(nr):
        cols = slice(i * LN, (i + 1) * LN)
        mi = stv[0:1, cols]
        buf[me, i:i + 1, :] = mi
        buf[me, nr + i:nr + i + 1, :] = stv[1:2, cols]
        T[i:i + 1, :] = stv[3:4, cols]
        tz = tz + jnp.where((lane + i * LN < n16) & (mi < SOME), stv[2:3, cols], 0.0)
    buf[me, 2 * nr:2 * nr + 8, :] = jnp.broadcast_to(tz, (8, LN))
    pl.semaphore_wait(barrier, n_vp - 1)
    copies = []
    for d in range(n_vp - 1):
        copies.append(pltpu.make_async_remote_copy(
            src_ref=buf.at[me], dst_ref=buf.at[me], send_sem=send.at[d], recv_sem=recv.at[d],
            device_id={"vp": lax.rem(me + d + 1, n_vp)}, device_id_type=pl.DeviceIdType.MESH))
    for c in copies:
        c.start()
    for c in copies:
        c.wait()
    m = buf[0, 0:nr, :]
    for p in range(1, n_vp):
        m = jnp.maximum(m, buf[p, 0:nr, :])
    s = jnp.zeros((nr, LN), F32)
    tz = jnp.zeros((1, LN), F32)
    for p in range(n_vp):
        s = s + buf[p, nr:2 * nr, :] * jnp.exp2(buf[p, 0:nr, :] - m)
        tz = tz + buf[p, 2 * nr:2 * nr + 1, :]
    lse = m + jnp.log(s) * LOG2E
    total = jnp.sum(jnp.where(live & (m < SOME), lse, 0.0)) - jnp.sum(tz)
    loss[...] = jnp.full((8, LN), total * (fs[0] * LN2), F32)
    L[0:nr, :] = lse + fs[1]


def stats_call(nr, n_dev, n_vp, R, cid, sc, fs, st):
    vm = pl.BlockSpec(memory_space=pltpu.VMEM)
    rows = jax.ShapeDtypeStruct((R // LN + 8, LN), F32)
    return pl.pallas_call(
        functools.partial(stats_kernel, nr, n_dev, n_vp),
        in_specs=[SMEM, SMEM, ANY],
        out_specs=[vm, vm, vm],
        out_shape=[rows, rows, jax.ShapeDtypeStruct((8, LN), F32)],
        scratch_shapes=[
            pltpu.VMEM((8, nr * LN), F32),
            pltpu.VMEM((n_vp, 2 * nr + 8, LN), F32),
            pltpu.SemaphoreType.DMA,
            pltpu.SemaphoreType.DMA((n_vp - 1,)),
            pltpu.SemaphoreType.DMA((n_vp - 1,)),
        ],
        compiler_params=pltpu.CompilerParams(collective_id=cid, has_side_effects=True, vmem_limit_bytes=VMEM_MOST // 2),
        name=f"stats{nr}",
    )(sc, fs, st)


def make_dz(zb, lt, i0, c0, lane, w, dst, jobs):
    for r, j in jobs:
        rs = slice(r * LN, (r + 1) * LN)
        cs = slice(j * LN, (j + 1) * LN)
        lr = jnp.broadcast_to(lt[0][pl.ds(i0 + r, 1), :], (LN, LN)).T
        trel = jnp.broadcast_to(lt[1][pl.ds(i0 + r, 1), :], (LN, LN)).T - (lane + c0)
        p = jnp.exp2(zb[rs, cs] - lr)
        dst[rs, cs] = (p - jnp.where(trel == float(j * LN), w, 0.0)).astype(BF16)


def dn_kernel(nch, n_dev, n_vp, D, V, sc, fs, L, T, z, w_hbm, dn, wb, zA, zB, dzA, dzB, acc, bsrc, brow, bgr, bcnt, dst, wsem, zsem, osem):
    NV = V // VB
    C = sum(CHS[:nch])
    w = fs[0]
    colf = sc[n_dev].astype(F32)
    dp = sc[n_dev + 1]
    lane = lax.broadcasted_iota(jnp.int32, (1, LN), 1).astype(F32)
    lt = (L, T)

    def wcopy(v):
        cols = pl.ds(mo(v * VB, VB), VB)
        return pltpu.make_async_copy(w_hbm.at[:, cols], wb.at[:, cols], wsem.at[v])

    wcopy(0).start()
    pos = jnp.int32(0)
    nblk = jnp.int32(0)
    n = jnp.int32(0)
    for c in range(nch):
        per = CHS[c] // GR
        g0 = sum(CHS[:c]) // GR
        start = pos
        mine = jnp.int32(0)
        for g in range(n_dev):
            qg = clip(granules(sc, g) - g0, 0, per)
            pos = pos + qg * GR
            start = start + jnp.where(g // n_vp < dp, qg * GR, 0)
            mine = mine + jnp.where(g // n_vp == dp, qg, 0)
        end = start + mine * GR
        low = start & -LN
        cnt = jnp.where(mine > 0, lax.shift_right_logical(end - low + BLK - 1, LB), 0)

        def fill(i, n, c=c, start=start, end=end, low=low, nblk=nblk):
            src = low + i * BLK
            lo = jnp.maximum(src, start)
            ng = lax.shift_right_logical(jnp.minimum(src + BLK, end) - lo, LG)
            bsrc[nblk + i] = src
            brow[nblk + i] = lo - src
            bgr[nblk + i] = n
            bcnt[nblk + i] = ng
            return n + ng

        n0 = n
        n = lax.fori_loop(0, cnt, fill, n)
        nblk = nblk + cnt
        for e in range(n_vp):
            qe = clip(granules(sc, dp * n_vp + e) - g0, 0, per)

            @pl.loop(0, qe)
            def _(i, g0=g0, e=e, n0=n0):
                dst[n0 + i] = e * C + (g0 + i) * GR
            n0 = n0 + qe

    def zcopy(b, vb, k):
        rows = pl.ds(mo(bsrc[b], LN), BLK)
        return pltpu.make_async_copy(z.at[rows, pl.ds(mo(vb * VB, VB), VB)], (zA, zB)[k], zsem.at[k])

    def ocopy(s, a, r):
        return pltpu.make_async_copy(acc.at[s, pl.ds(mo(a, GR), GR), :], dn.at[pl.ds(mo(r, GR), GR), :], osem.at[s])

    def ostart(b, s):
        @pl.loop(0, bcnt[b])
        def _(i):
            ocopy(s, brow[b] + i * GR, dst[bgr[b] + i]).start()

    def owait(b, s):
        @pl.loop(0, bcnt[b])
        def _(i):
            ocopy(s, 0, 0).wait()

    NR = BLK // LN
    NC = D // 512

    @pl.when(nblk == 0)
    def _():
        wcopy(0).wait()

    @pl.when(nblk > 0)
    def _():
        zcopy(0, 0, 0).start()
        zcopy(0, 1, 1).start()
        for v in range(1, NV):
            wcopy(v).start()
        zcopy(0, 0, 0).wait()
        everything = [(r, j) for r in range(NR) for j in range(VB // LN)]
        make_dz(zA, lt, lax.shift_right_logical(bsrc[0], LB - 2), colf, lane, w, dzA, everything)
        step = -(-len(everything) // (NC - 1))

        def half(b, vb, wraps, cur, nxt, k):
            s = b & 1
            first = vb == 0
            nb = jnp.minimum(b + jnp.where(wraps, 1, 0), nblk - 1)
            nvb = jnp.where(wraps, 0, vb + 1)

            @pl.when(jnp.logical_not(wraps) | (b + 1 < nblk))
            def _():
                zcopy(0, 0, k).wait()
            v2 = vb + 2
            over = v2 >= NV
            b2 = b + jnp.where(over, 1, 0)

            @pl.when(b2 < nblk)
            def _():
                zcopy(b2, jnp.where(over, v2 - NV, v2), 1 - k).start()

            @pl.when(first & (b >= 2))
            def _():
                owait(b - 2, s)

            @pl.when(b == 0)
            def _():
                wcopy(vb).wait()
            c0 = colf + (nvb * VB).astype(F32)
            i0 = lax.shift_right_logical(bsrc[nb], LB - 2)

            def run(rows):
                for q in range(NC):
                    cs = slice(q * 512, (q + 1) * 512)
                    y = lax.dot_general(cur[0:rows, :], wb[cs, pl.ds(mo(vb * VB, VB), VB)], (((1,), (1,)), ((), ())), preferred_element_type=F32)
                    acc[s, 0:rows, cs] = jnp.where(first, 0.0, acc[s, 0:rows, cs]) + y
                    make_dz((zA, zB)[k], lt, i0, c0, lane, w, nxt, everything[q * step:(q + 1) * step])

            small = brow[b] + bcnt[b] * GR <= BLK // 2

            @pl.when(small)
            def _():
                run(BLK // 2)

            @pl.when(jnp.logical_not(small))
            def _():
                run(BLK)

            @pl.when(wraps)
            def _():
                ostart(b, s)

        @pl.loop(0, nblk)
        def _(b):
            @pl.loop(0, NV // 2)
            def _(v):
                half(b, 2 * v, jnp.bool_(False), dzA, dzB, 1)
                half(b, 2 * v + 1, v == NV // 2 - 1, dzB, dzA, 0)

        @pl.when(nblk >= 2)
        def _():
            owait(nblk - 2, nblk & 1)
        owait(nblk - 1, (nblk - 1) & 1)


def dn_call(nch, n_dev, n_vp, D, V, sc, fs, L, T, z, w):
    dma = pltpu.SemaphoreType.DMA
    vm = pl.BlockSpec(memory_space=pltpu.VMEM)
    table = pltpu.SMEM((64,), jnp.int32)
    return pl.pallas_call(
        functools.partial(dn_kernel, nch, n_dev, n_vp, D, V),
        in_specs=[SMEM, SMEM, vm, vm, ANY, ANY],
        out_specs=ANY,
        out_shape=jax.ShapeDtypeStruct((n_vp * sum(CHS[:nch]), D), F32),
        scratch_shapes=[
            pltpu.VMEM((D, V), BF16),
            pltpu.VMEM((BLK, VB), F32),
            pltpu.VMEM((BLK, VB), F32),
            pltpu.VMEM((BLK, VB), BF16),
            pltpu.VMEM((BLK, VB), BF16),
            pltpu.VMEM((2, BLK, D), F32),
            table, table, table, table,
            pltpu.SMEM((n_vp * sum(CHS[:nch]) // GR,), jnp.int32),
            dma((V // VB,)), dma((2,)), dma((2,)),
        ],
        compiler_params=pltpu.CompilerParams(vmem_limit_bytes=VMEM_MOST),
        cost_estimate=pl.CostEstimate(flops=n_vp * sum(CHS[:nch]) * D * V, bytes_accessed=D * V * 2, transcendentals=0),
        name=f"dn{nch}",
    )(sc, fs, L, T, z, w)


def dw_kernel(n_dev, D, V, sc, fs, L, T, nT, z, dw, nb, zA, zB, dzA, dzB, acc, nsem, zsem, osem):
    NT = V // TN3
    w = fs[0]
    colf = sc[n_dev].astype(F32)
    lane = lax.broadcasted_iota(jnp.int32, (1, LN), 1).astype(F32)
    lt = (L, T)
    g16 = jnp.int32(0)
    for g in range(n_dev):
        g16 = g16 + granules(sc, g)
    nb512 = lax.shift_right_logical(g16 * GR + BLK - 1, LB)
    S = lax.shift_right_logical(nb512 + 1, 1)
    odd = nb512 & 1
    NR = KT // LN

    def ncopy(t):
        cols = pl.ds(mo(t * BLK, BLK), BLK)
        return pltpu.make_async_copy(nT.at[:, cols], nb.at[:, cols], nsem.at[t])

    def is_half(t):
        return (t == S - 1) & (odd == 1)

    def zgo(ct, t, k, start):
        h = is_half(t)
        for size, cond in ((KT, jnp.logical_not(h)), (BLK, h)):
            @pl.when(cond)
            def _(size=size):
                cols = pl.ds(mo(ct * TN3, TN3), TN3)
                c = pltpu.make_async_copy(z.at[pl.ds(mo(t * KT, KT), size), cols], (zA, zB)[k].at[pl.ds(0, size), :], zsem.at[k])
                if start:
                    c.start()
                else:
                    c.wait()

    def nxt(ct, t):
        wrap = t + 1 == S
        return ct + jnp.where(wrap, 1, 0), jnp.where(wrap, 0, t + 1)

    def ocopy(ct, s):
        return pltpu.make_async_copy(acc.at[s], dw.at[:, pl.ds(mo(ct * TN3, TN3), TN3)], osem.at[s])

    MS = 512
    NM = D // MS
    zero = jnp.int32(0)
    zgo(zero, zero, 0, True)
    c1, t1 = nxt(zero, zero)
    zgo(c1, t1, 1, True)

    @pl.loop(0, nb512)
    def _(t):
        ncopy(t).start()
    zgo(zero, zero, 0, False)
    jobs = [(r, j) for r in range(NR) for j in range(TN3 // LN)]
    make_dz(zA, lt, zero, colf, lane, w, dzA, jobs)
    step = -(-len(jobs) // (NM - 1))
    c2, t2 = nxt(c1, t1)
    zgo(c2, t2, 0, True)

    def half(ct, t, cur, nxtbuf, k):
        s = ct & 1
        na, ta = nxt(ct, t)
        nb_, tb_ = nxt(na, ta)
        nc, tc = nxt(nb_, tb_)

        @pl.when(na < NT)
        def _():
            zgo(na, ta, k, False)

        @pl.when(ct == 0)
        def _():
            ncopy(2 * t).wait()

            @pl.when(jnp.logical_not(is_half(t)))
            def _():
                ncopy(2 * t + 1).wait()

        @pl.when((t == 0) & (ct >= 2))
        def _():
            ocopy(0, s).wait()
        c0 = colf + (na * TN3).astype(F32)
        i0 = ta * NR
        first = t == 0

        def run(size):
            cols = pl.ds(mo(t * KT, KT), size)
            for m in range(NM):
                ms = slice(m * MS, (m + 1) * MS)
                y = jnp.dot(nb[ms, cols], cur[0:size, :], preferred_element_type=F32)
                acc[s, ms, :] = jnp.where(first, 0.0, acc[s, ms, :]) + y
                make_dz((zA, zB)[k], lt, i0, c0, lane, w, nxtbuf, jobs[m * step:(m + 1) * step])

        h = is_half(t)

        @pl.when(jnp.logical_not(h))
        def _():
            run(KT)

        @pl.when(h)
        def _():
            run(BLK)

        @pl.when(nc < NT)
        def _():
            zgo(nc, tc, k, True)

        @pl.when(t == S - 1)
        def _():
            ocopy(ct, s).start()
        return na, ta

    def pair(i, carry):
        ct, t = carry
        ct, t = half(ct, t, dzA, dzB, 1)
        return half(ct, t, dzB, dzA, 0)

    lax.fori_loop(0, S * (NT // 2), pair, (zero, zero))
    ocopy(0, 0).wait()
    ocopy(0, 1).wait()


def dw_call(n_dev, D, V, R, rows_est, sc, fs, L, T, nT, z):
    dma = pltpu.SemaphoreType.DMA
    vm = pl.BlockSpec(memory_space=pltpu.VMEM)
    return pl.pallas_call(
        functools.partial(dw_kernel, n_dev, D, V),
        in_specs=[SMEM, SMEM, vm, vm, ANY, ANY],
        out_specs=ANY,
        out_shape=jax.ShapeDtypeStruct((D, V), F32),
        scratch_shapes=[
            pltpu.VMEM((D, R), BF16),
            pltpu.VMEM((KT, TN3), F32),
            pltpu.VMEM((KT, TN3), F32),
            pltpu.VMEM((KT, TN3), BF16),
            pltpu.VMEM((KT, TN3), BF16),
            pltpu.VMEM((2, D, TN3), F32),
            dma((R // BLK,)), dma((2,)), dma((2,)),
        ],
        compiler_params=pltpu.CompilerParams(vmem_limit_bytes=VMEM_MOST),
        cost_estimate=pl.CostEstimate(flops=2 * rows_est * D * V, bytes_accessed=D * V * 4, transcendentals=0),
        name="dw",
    )(sc, fs, L, T, nT, z)


def total_kernel(n_dp, n_vp, part, out, buf, sem, send, recv):
    n = n_dp * n_vp
    me = lax.axis_index("dp") * n_vp + lax.axis_index("vp")
    barrier = pltpu.get_barrier_semaphore()
    own = pltpu.make_async_copy(part, buf.at[me], sem)
    own.start()

    def peer(d):
        t = lax.rem(me + d, n)
        return {"dp": t // n_vp, "vp": lax.rem(t, n_vp)}

    for d in range(1, n):
        pl.semaphore_signal(barrier, inc=1, device_id=peer(d), device_id_type=pl.DeviceIdType.MESH)
    own.wait()
    pl.semaphore_wait(barrier, n - 1)
    copies = [
        pltpu.make_async_remote_copy(
            src_ref=buf.at[me], dst_ref=buf.at[me], send_sem=send.at[d - 1], recv_sem=recv.at[d - 1],
            device_id=peer(d), device_id_type=pl.DeviceIdType.MESH)
        for d in range(1, n)
    ]
    for c in copies:
        c.start()
    for c in copies:
        c.wait()
    acc = buf[0]
    for p in range(1, n):
        acc = acc + buf[p]
    out[...] = acc


def total_call(n_dp, n_vp, part):
    n = n_dp * n_vp
    return pl.pallas_call(
        functools.partial(total_kernel, n_dp, n_vp),
        in_specs=[ANY],
        out_specs=pl.BlockSpec(memory_space=pltpu.VMEM),
        out_shape=jax.ShapeDtypeStruct(part.shape, F32),
        scratch_shapes=[
            pltpu.VMEM((n, *part.shape), F32),
            pltpu.SemaphoreType.DMA,
            pltpu.SemaphoreType.DMA((n - 1,)),
            pltpu.SemaphoreType.DMA((n - 1,)),
        ],
        compiler_params=pltpu.CompilerParams(collective_id=len(CHS) + 1, has_side_effects=True),
        name="total",
    )(part)


def solution(mesh):
    n_vp = mesh.shape["vp"]
    n_dp = mesh.shape["dp"]
    n_dev = n_vp * n_dp

    def local_step(hidden, targets, loss_mask, norm_scale, w_head):
        D, V = w_head.shape
        tok = hidden.shape[1]
        R = n_dev * tok
        x = hidden[0]
        x_f32 = x.astype(F32)
        inv_rms = lax.rsqrt(jnp.mean(x_f32 * x_f32, axis=-1, keepdims=True) + EPS)
        normed = (x_f32 * inv_rms * norm_scale).astype(BF16)
        keep = loss_mask[0] > 0
        keep_b = keep.astype(BF16)
        before = (lax.broadcasted_iota(jnp.int32, (tok, tok), 1) >= lax.broadcasted_iota(jnp.int32, (tok, tok), 0)).astype(BF16)
        rank = jnp.dot(keep_b[None, :], before, preferred_element_type=F32)[0].astype(jnp.int32) - 1
        slot = lax.broadcasted_iota(jnp.int32, (tok, tok), 0)
        perm = ((slot == rank[None, :]) & keep[None, :]).astype(BF16)
        cuts = [sum(CHS[:i]) for i in range(len(CHS) + 1)]
        sent = [jnp.dot(perm[a:b], normed, preferred_element_type=F32) for a, b in zip(cuts, cuts[1:])]
        tgt = targets[0]
        pair = jnp.stack([(tgt // 256).astype(BF16), (tgt % 256).astype(BF16), keep_b], axis=1)
        got = jnp.dot(perm, pair, preferred_element_type=F32)
        meta = jnp.where(got[:, 2] > 0.5, got[:, 0] * 256.0 + got[:, 1], -1.0)

        def gather(c):
            return lax.all_gather(sent[c], ("dp", "vp"), axis=0, tiled=False)

        chunk0 = gather(0)
        metas = lax.all_gather(meta, ("dp", "vp"), axis=0, tiled=False)
        counts = jnp.sum((metas >= 0.0).astype(jnp.int32), axis=1)
        count = jnp.sum(counts).astype(F32)
        weight = 1.0 / count
        sc = jnp.concatenate([counts, jnp.stack([lax.axis_index("vp") * V, lax.axis_index("dp")])]).astype(jnp.int32)
        fs = jnp.stack([weight, jnp.log(count) * LOG2E])
        metab = jnp.broadcast_to(metas[:, :, None], (n_dev, tok, LN))
        most = jnp.max(counts)
        branch = sum((most > c).astype(jnp.int32) for c in cuts[1:-1])

        def make(nch):
            def run(chunk0, sent, metab, sc, fs, w_head, x, perm, norm_scale, meta):
                chunks = [chunk0] + [lax.all_gather(v, ("dp", "vp"), axis=0, tiled=False) for v in sent[:nch - 1]]
                state = None
                for c in range(nch):
                    state = logits_call(c, c == 0, c == nch - 1, n_dev, D, V, R, sc, chunks[c], metab, w_head, state)
                z, nT, st = state[:3]
                C = cuts[nch]
                L, T, loss = stats_call(-(-C * n_dev // (8 * LN)) * 8, n_dev, n_vp, R, nch, sc, fs, st)
                dn = dn_call(nch, n_dev, n_vp, D, V, sc, fs, L, T, z, w_head)
                d_normed = lax.psum_scatter(dn, "vp", scatter_dimension=0, tiled=True)
                d_w = dw_call(n_dev, D, V, R, n_dev * C // 2, sc, fs, L, T, nT, z)
                xc = jnp.dot(perm[:C], x, preferred_element_type=F32)
                live = (meta[:C] >= 0.0)[:, None]
                rc = lax.rsqrt(jnp.mean(xc * xc, axis=-1, keepdims=True) + EPS)
                xh = xc * rc
                d_normed = jnp.where(live, d_normed, 0.0)
                d_scale = jnp.sum(d_normed * xh, axis=0)
                e = d_normed * norm_scale
                dx = rc * (e - xh * jnp.mean(e * xh, axis=-1, keepdims=True))
                d_hidden = lax.dot_general(perm[:C], dx.astype(BF16), (((0,), (0,)), ((), ())), preferred_element_type=F32).astype(BF16)
                return loss[0, 0], d_hidden, d_w, d_scale
            return run

        loss, d_hidden, d_w, d_scale = lax.switch(
            branch, [make(i + 1) for i in range(len(CHS))],
            chunk0, sent[1:], metab, sc, fs, w_head, x, perm, norm_scale, meta)
        part = jnp.pad(d_scale.reshape(-1, LN), ((0, -(D // LN) % 8), (0, 0)))
        d_scale = total_call(n_dp, n_vp, part)[:D // LN].reshape(D)
        return loss, d_hidden[None], d_w, d_scale

    return jax.shard_map(
        local_step,
        mesh=mesh,
        in_specs=(P("dp", "vp", None), P("dp", "vp"), P("dp", "vp"), P(None), P(None, "vp")),
        out_specs=(P(), P("dp", "vp", None), P(None, "vp"), P(None)),
        check_vma=False,
    )
```
